32 devices in a mesh: gx: 2 (over x), gy: 4 (over z), gz: 4 (over y, core).
Axes of the slice: x: 2, y: 2, z: 4, core: 2. Of those that a mesh axis runs over, the one named last changes fastest.
Arguments:
- acts: bfloat16 [40960, 768], P(('gx', 'gy', 'gz')), may hold values from -6 to 6
- grads_out: bfloat16 [40960, 768], P(('gx', 'gy', 'gz')), may hold values from -0.03125 to 0.03125
- master: float32 [4608, 128], P(('gx', 'gy', 'gz')), may hold values from -0.3 to 0.3
- moment: float32 [4608, 128], P(('gx', 'gy', 'gz')), may hold values from -6 to 6
- second: float32 [4608, 128], P(('gx', 'gy', 'gz')), may hold values from 0.1 to 2
Outputs:
- master_new: float32 [4608, 128], P(('gx', 'gy', 'gz'))
- moment_new: float32 [4608, 128], P(('gx', 'gy', 'gz'))
- second_new: float32 [4608, 128], P(('gx', 'gy', 'gz'))
- weights: bfloat16 [768, 768], replicated
The draws below stay inside these ranges and needn't reach their ends.
All inputs are finite; a program needn't handle non-finite values.
Results may differ from the reference program's by a relative error of at most 0.003.
Values may be sent and summed in bfloat16 or wider, within the bound.
No kernel may reach another device: no remote copies, remote signals or barrier semaphores. Data moves between devices by JAX's collectives and lax.ppermute only.
A program may use at most 64 MiB of HBM per device.

```python
import math
import jax
import jax.numpy as jnp
from jax import lax

IN = 768
OUT = 768
LANE = 128
STEP = 1000
TOK_DEV = 1280
TOKENS = 40960
FLAT = 4608


def spiked(result, own_key, source, target, shards_of, factor):
    def block_of(position):
        return (jnp.arange(result.shape[position]) // (result.shape[position] // shards_of)).reshape((-1,) + (1,) * (result.ndim - 1 - position))

    one_side = jax.random.permutation(own_key, shards_of)[block_of(target)]
    far = (block_of(target) + shards_of // 2) % shards_of
    return jnp.where((block_of(source) == one_side) | (block_of(source) == far), factor * result, result)


def block_levels(key, extent, cuts, least, top_value):
    gain, own = 1.0, jax.random.fold_in(key, 6)
    for dim, blocks in cuts:
        steps = jnp.exp(jax.random.uniform(jax.random.fold_in(own, dim), (blocks,), jnp.float32, least / len(cuts), top_value / len(cuts)))
        gain = gain * jnp.repeat(steps, extent[dim] // blocks).reshape([-1 if axis == dim else 1 for axis in range(len(extent))])
    return gain


def noise(own_key, shape, width, reach, shards=(), held_as=jnp.bfloat16):
    drawn = jax.random.normal(own_key, shape, jnp.float32) * width
    if len(shards) > 0:
        drawn = block_levels(own_key, shape, shards, -0.22, 0.18) * drawn
    return jnp.clip(drawn, min=-reach, max=reach).astype(held_as)


def gaussian_with(rng, shape, spread, reach, pieces, heavy, kind=jnp.bfloat16):
    array = spread * jax.random.normal(rng, shape, jnp.float32)
    if pieces:
        array = array * block_levels(rng, shape, pieces, -0.22, 0.18)
    return jnp.clip(spiked(array, jax.random.fold_in(rng, 3), *heavy), -reach, reach).astype(kind)


def setup_inputs(seed: int = 0) -> dict:
    keys = jax.random.split(jax.random.key(seed), 6)
    return {
        "acts": gaussian_with(keys[0], (TOKENS, IN), 1.0, 6.0, ((0, 32),), (0, 1, 32, 2.75)),
        "grads_out": noise(keys[1], (TOKENS, OUT), TOKENS ** -0.5, 0.03125, ((0, 32),)),
        "master": noise(keys[2], (FLAT, LANE), 0.05, 0.3, ((0, 32),), jnp.float32),
        "moment": noise(keys[3], (FLAT, LANE), 1.0, 6.0, ((0, 32),), jnp.float32),
        "second": jnp.clip(jnp.exp(math.log(2.0) - 2.9957323 * jax.random.uniform(keys[4], (FLAT, LANE), jnp.float32) ** block_levels(keys[4], (FLAT, LANE), ((0, 32),), -0.2, 0.2)), 0.1, 2.0),
    }


def reference(acts, grads_out, master, moment, second):
    blocks = TOKENS // TOK_DEV
    act_blocks = acts.reshape(blocks, TOK_DEV, IN)
    cot_blocks = grads_out.reshape(blocks, TOK_DEV, OUT)

    def add_block(total, pair):
        product = lax.dot_general(pair[0], pair[1], (((0,), (0,)), ((), ())), preferred_element_type=jnp.float32)
        return (total + product, None)
    start = jnp.zeros((IN, OUT), jnp.float32)
    gradient, _ = lax.scan(add_block, start, (act_blocks, cot_blocks))
    gradient = gradient.reshape(FLAT, LANE)
    moment_new = 0.9 * moment + 0.1 * gradient
    second_new = 0.95 * second + 0.05 * gradient * gradient
    first_fix = 1.0 - 0.9 ** STEP
    second_fix = 1.0 - 0.95 ** STEP
    ratio = moment_new / first_fix / (jnp.sqrt(second_new / second_fix) + 1e-08)
    master_new = master - 0.01 * (ratio + 0.01 * master)
    weights = master_new.astype(jnp.bfloat16).reshape(IN, OUT)
    return (master_new, moment_new, second_new, weights)
```

```python
import functools

import jax
import jax.numpy as jnp
from jax import lax
from jax.experimental import pallas as pl
from jax.experimental.pallas import tpu as pltpu
from jax.sharding import Mesh, PartitionSpec as P

STEP = 1000
AXES = ("gx", "gy", "gz")
SPLIT = ("gx", "gy", "gr", "gc")
BF16, F32 = jnp.bfloat16, jnp.float32
VMEM = pl.BlockSpec(memory_space=pltpu.VMEM)
ANY = pl.BlockSpec(memory_space=pl.ANY)


def adam(gradient, master, moment, second):
    moment_new = 0.9 * moment + 0.1 * gradient
    second_new = 0.95 * second + 0.05 * gradient * gradient
    first_fix = 1.0 - 0.9**STEP
    second_fix = 1.0 - 0.95**STEP
    ratio = moment_new / first_fix / (jnp.sqrt(second_new / second_fix) + 1e-08)
    master_new = master - 0.01 * (ratio + 0.01 * master)
    return master_new, moment_new, second_new


def shards(acts, grads_out, master, moment, second):
    width_in = acts.shape[1]
    width_out = grads_out.shape[1]
    lane = master.shape[1]
    total_rows = width_in * width_out // lane
    local_grad = lax.dot_general(
        acts, grads_out, (((0,), (0,)), ((), ())), preferred_element_type=F32
    )
    value = local_grad.reshape(total_rows, lane)
    for axis in AXES:
        value = lax.psum_scatter(
            value.astype(BF16), axis, scatter_dimension=0, tiled=True
        ).astype(F32)
    master_new, moment_new, second_new = adam(value, master, moment, second)
    gathered = master_new.astype(BF16)
    for axis in AXES[::-1]:
        gathered = lax.all_gather(gathered, axis, axis=0, tiled=True)
    return (master_new, moment_new, second_new, gathered.reshape(width_in, width_out))


def here():
    return tuple(lax.axis_index(axis) for axis in SPLIT)


def struct(shape, dtype):
    return jax.ShapeDtypeStruct(shape, dtype)


def matmul_kernel(sizes, rows, a, g, send, keep):
    nx, nz, nr = sizes
    mx, mz, mr, mc = here()
    product = lax.dot_general(
        a[...], g[...], (((0,), (0,)), ((), ())), preferred_element_type=F32
    ).astype(BF16)

    def place(own):
        for block in range(nx * nz * nr * 2):
            c, r = block % 2, block // 2 % nr
            z, x = block // (2 * nr) % nz, block // (2 * nr * nz)
            target = keep if c == own else send
            target[(x ^ mx) * nr + (r ^ mr), z ^ mz] = product[
                rows * block : rows * (block + 1)
            ]

    for own in range(2):
        pl.when(mc == own)(functools.partial(place, own))


def split_kernel(n_in, kept, *refs):
    arrivals, pieces = refs[:n_in], refs[n_in:]
    for k, piece in enumerate(pieces):
        total = kept[k].astype(F32)
        for arrival in arrivals:
            total += arrival[k].astype(F32)
        piece[...] = total.astype(piece.dtype)


def split(name, kept, arrivals):
    n, shape = kept.shape[0], kept.shape[1:]
    return pl.pallas_call(
        functools.partial(split_kernel, len(arrivals)),
        in_specs=[VMEM] * (1 + len(arrivals)),
        out_specs=[VMEM] * n,
        out_shape=[struct(shape, F32)] + [struct(shape, BF16)] * (n - 1),
        name=name,
    )(kept, *arrivals)


def adam_kernel(n_in, rows, per_row, lane, kept, *refs):
    arrivals = refs[:n_in]
    master, moment, second = refs[n_in : n_in + 3]
    master_new, moment_new, second_new, weights, flat = refs[n_in + 3 :]
    total = kept[...].astype(F32)
    for arrival in arrivals:
        total += arrival[...].astype(F32)
    for j in range(per_row):
        flat[pl.ds(j, rows, stride=per_row), :] = total[:, j * lane : (j + 1) * lane]
    values = adam(flat[...], master[...], moment[...], second[...])
    master_new[...], moment_new[...], second_new[...] = values
    flat[...] = values[0]
    for j in range(per_row):
        weights[:, j * lane : (j + 1) * lane] = flat[
            pl.ds(j, rows, stride=per_row), :
        ].astype(BF16)


def stack_kernel(axis, *refs):
    pieces, out = refs[:-1], refs[-1]
    me = lax.axis_index(axis)
    for k, piece in enumerate(pieces):
        out[me ^ k] = piece[...]


def place_kernel(sizes, rows, own, other, out, sem):
    nx, nz, nr = sizes
    mc = lax.axis_index("gc")

    def copies(first):
        for block in range(nx * nz * nr * 2):
            c, r = block % 2, block // 2 % nr
            z, x = block // (2 * nr) % nz, block // (2 * nr * nz)
            source = own if c == first else other
            yield pltpu.make_async_copy(
                source.at[x * nr + r, z], out.at[pl.ds(rows * block, rows)], sem
            )

    def run(first):
        for copy in copies(first):
            copy.start()
        for copy in copies(first):
            copy.wait()

    for first in range(2):
        pl.when(mc == first)(functools.partial(run, first))


def fast(sizes, acts, grads_out, master, moment, second):
    nx, nz, nr = sizes
    width_in, width_out = acts.shape[1], grads_out.shape[1]
    own_rows, lane = master.shape
    per_row = width_out // lane
    rows = own_rows // per_row
    group = nx * nr

    def permute(value, dx=0, dz=0, dr=0, dc=0):
        pairs = []
        for x in range(nx):
            for z in range(nz):
                for r in range(nr):
                    for c in range(2):
                        source = ((x * nz + z) * nr + r) * 2 + c
                        target = (((x ^ dx) * nz + (z ^ dz)) * nr + (r ^ dr)) * 2
                        pairs.append((source, target + (c ^ dc)))
        return lax.ppermute(value, SPLIT, pairs)

    half = struct((group, nz, rows, width_out), BF16)
    send, keep = pl.pallas_call(
        functools.partial(matmul_kernel, sizes, rows),
        in_specs=[VMEM] * 2,
        out_specs=[VMEM] * 2,
        out_shape=[half] * 2,
        name="matmul",
    )(acts, grads_out)
    kept, *pieces = split("split_core", keep, [permute(send, dc=1)])
    arrivals = [
        permute(piece, dx=k // nr, dr=k % nr) for k, piece in enumerate(pieces, 1)
    ]
    kept, *pieces = split("split_plane", kept, arrivals)
    arrivals = [permute(piece, dz=k) for k, piece in enumerate(pieces, 1)]
    state = struct((own_rows, lane), F32)
    master_new, moment_new, second_new, weights = pl.pallas_call(
        functools.partial(adam_kernel, len(arrivals), rows, per_row, lane),
        in_specs=[VMEM] * (4 + len(arrivals)),
        out_specs=[VMEM] * 4,
        out_shape=[state] * 3 + [struct((rows, width_out), BF16)],
        scratch_shapes=[pltpu.VMEM((own_rows, lane), F32)],
        name="adam",
    )(kept, *arrivals, master, moment, second)
    line = pl.pallas_call(
        functools.partial(stack_kernel, "gy"),
        in_specs=[VMEM] * nz,
        out_specs=VMEM,
        out_shape=struct((nz, rows, width_out), BF16),
        name="stack_line",
    )(weights, *[permute(weights, dz=k) for k in range(1, nz)])
    own = lax.all_gather(line, ("gx", "gr"), axis=0)
    out = pl.pallas_call(
        functools.partial(place_kernel, sizes, rows),
        in_specs=[ANY] * 2,
        out_specs=ANY,
        out_shape=struct((width_in, width_out), BF16),
        scratch_shapes=[pltpu.SemaphoreType.DMA],
        name="place",
    )(own, permute(own, dc=1))
    return master_new, moment_new, second_new, out


def power_of_two(n):
    return n & (n - 1) == 0


def chosen(mesh, sizes, *args):
    acts, grads_out, master = args[:3]
    width_in, width_out = acts.shape[1], grads_out.shape[1]
    even = all(power_of_two(n) for n in sizes) and mesh.shape["gz"] % 2 == 0
    whole = width_in % (8 * mesh.size) == 0 and width_out % master.shape[1] == 0
    if not (even and whole):
        spec = P(AXES, None)
        return jax.shard_map(
            shards, mesh=mesh, in_specs=(spec,) * 5,
            out_specs=(spec,) * 3 + (P(),), check_vma=False,
        )(*args)
    spec = P(SPLIT, None)
    finer = Mesh(mesh.devices.reshape(*sizes, 2), SPLIT)
    return jax.shard_map(
        functools.partial(fast, sizes), mesh=finer, in_specs=(spec,) * 5,
        out_specs=(spec,) * 3 + (P(),), check_vma=False,
    )(*args)


def solution(mesh):
    sizes = (mesh.shape["gx"], mesh.shape["gy"], mesh.shape["gz"] // 2)
    return functools.partial(chosen, mesh, sizes)
```

```python
import functools

import jax
import jax.numpy as jnp
from jax import lax
from jax.experimental import pallas as pl
from jax.experimental.pallas import tpu as pltpu
from jax.sharding import Mesh, PartitionSpec as P

STEP = 1000
AXES = ("gx", "gy", "gz")
SPLIT = ("gx", "gy", "gr", "gc")
BF16, F32 = jnp.bfloat16, jnp.float32
VMEM = pl.BlockSpec(memory_space=pltpu.VMEM)
ANY = pl.BlockSpec(memory_space=pl.ANY)


def adam(gradient, master, moment, second):
    moment_new = 0.9 * moment + 0.1 * gradient
    second_new = 0.95 * second + 0.05 * gradient * gradient
    first_fix = 1.0 - 0.9**STEP
    second_fix = 1.0 - 0.95**STEP
    ratio = moment_new / first_fix / (jnp.sqrt(second_new / second_fix) + 1e-08)
    master_new = master - 0.01 * (ratio + 0.01 * master)
    return master_new, moment_new, second_new


def shards(acts, grads_out, master, moment, second):
    width_in = acts.shape[1]
    width_out = grads_out.shape[1]
    lane = master.shape[1]
    total_rows = width_in * width_out // lane
    local_grad = lax.dot_general(
        acts, grads_out, (((0,), (0,)), ((), ())), preferred_element_type=F32
    )
    value = local_grad.reshape(total_rows, lane)
    for axis in AXES:
        value = lax.psum_scatter(
            value.astype(BF16), axis, scatter_dimension=0, tiled=True
        ).astype(F32)
    master_new, moment_new, second_new = adam(value, master, moment, second)
    gathered = master_new.astype(BF16)
    for axis in AXES[::-1]:
        gathered = lax.all_gather(gathered, axis, axis=0, tiled=True)
    return (master_new, moment_new, second_new, gathered.reshape(width_in, width_out))


def here():
    return tuple(lax.axis_index(axis) for axis in SPLIT)


def near(*arrays):
    return [pltpu.with_memory_space_constraint(a, pltpu.VMEM) for a in arrays]


def struct(shape, dtype):
    return pltpu.VMEM(shape, dtype)


def matmul_kernel(sizes, rows, a, g, send, keep):
    nx, nz, nr = sizes
    mx, mz, mr, mc = here()
    product = lax.dot_general(
        a[...], g[...], (((0,), (0,)), ((), ())), preferred_element_type=F32
    ).astype(BF16)

    def place(own):
        for block in range(nx * nz * nr * 2):
            c, r = block % 2, block // 2 % nr
            z, x = block // (2 * nr) % nz, block // (2 * nr * nz)
            target = keep if c == own else send
            target[(x ^ mx) * nr + (r ^ mr), z ^ mz] = product[
                rows * block : rows * (block + 1)
            ]

    for own in range(2):
        pl.when(mc == own)(functools.partial(place, own))


def split_kernel(n_in, kept, *refs):
    arrivals, pieces = refs[:n_in], refs[n_in:]
    for k, piece in enumerate(pieces):
        total = kept[k].astype(F32)
        for arrival in arrivals:
            total += arrival[k].astype(F32)
        piece[...] = total.astype(piece.dtype)


def split(name, kept, arrivals):
    n, shape = kept.shape[0], kept.shape[1:]
    return pl.pallas_call(
        functools.partial(split_kernel, len(arrivals)),
        in_specs=[VMEM] * (1 + len(arrivals)),
        out_specs=[VMEM] * n,
        out_shape=[struct(shape, F32)] + [struct(shape, BF16)] * (n - 1),
        name=name,
    )(*near(kept, *arrivals))


def adam_kernel(n_in, rows, per_row, lane, kept, *refs):
    arrivals = refs[:n_in]
    master, moment, second = refs[n_in : n_in + 3]
    master_new, moment_new, second_new, weights, flat = refs[n_in + 3 :]
    total = kept[...].astype(F32)
    for arrival in arrivals:
        total += arrival[...].astype(F32)
    for j in range(per_row):
        flat[pl.ds(j, rows, stride=per_row), :] = total[:, j * lane : (j + 1) * lane]
    values = adam(flat[...], master[...], moment[...], second[...])
    master_new[...], moment_new[...], second_new[...] = values
    flat[...] = values[0]
    for j in range(per_row):
        weights[:, j * lane : (j + 1) * lane] = flat[
            pl.ds(j, rows, stride=per_row), :
        ].astype(BF16)


def stack_kernel(axis, *refs):
    pieces, out = refs[:-1], refs[-1]
    me = lax.axis_index(axis)
    for k, piece in enumerate(pieces):
        out[me ^ k] = piece[...]


def place_kernel(sizes, rows, own, other, out, sem):
    nx, nz, nr = sizes
    mc = lax.axis_index("gc")

    def copies(first):
        for block in range(nx * nz * nr * 2):
            c, r = block % 2, block // 2 % nr
            z, x = block // (2 * nr) % nz, block // (2 * nr * nz)
            source = own if c == first else other
            yield pltpu.make_async_copy(
                source.at[x * nr + r, z], out.at[pl.ds(rows * block, rows)], sem
            )

    def run(first):
        for copy in copies(first):
            copy.start()
        for copy in copies(first):
            copy.wait()

    for first in range(2):
        pl.when(mc == first)(functools.partial(run, first))


def fast(sizes, acts, grads_out, master, moment, second):
    nx, nz, nr = sizes
    width_in, width_out = acts.shape[1], grads_out.shape[1]
    own_rows, lane = master.shape
    per_row = width_out // lane
    rows = own_rows // per_row
    group = nx * nr

    def permute(value, dx=0, dz=0, dr=0, dc=0):
        pairs = []
        for x in range(nx):
            for z in range(nz):
                for r in range(nr):
                    for c in range(2):
                        source = ((x * nz + z) * nr + r) * 2 + c
                        target = (((x ^ dx) * nz + (z ^ dz)) * nr + (r ^ dr)) * 2
                        pairs.append((source, target + (c ^ dc)))
        return lax.ppermute(value, SPLIT, pairs)

    half = struct((group, nz, rows, width_out), BF16)
    send, keep = pl.pallas_call(
        functools.partial(matmul_kernel, sizes, rows),
        in_specs=[VMEM] * 2,
        out_specs=[VMEM] * 2,
        out_shape=[half] * 2,
        name="matmul",
    )(acts, grads_out)
    kept, *pieces = split("split_core", keep, [permute(send, dc=1)])
    arrivals = [
        permute(piece, dx=k // nr, dr=k % nr) for k, piece in enumerate(pieces, 1)
    ]
    kept, *pieces = split("split_plane", kept, arrivals)
    arrivals = [permute(piece, dz=k) for k, piece in enumerate(pieces, 1)]
    state = jax.ShapeDtypeStruct((own_rows, lane), F32)
    master_new, moment_new, second_new, weights = pl.pallas_call(
        functools.partial(adam_kernel, len(arrivals), rows, per_row, lane),
        in_specs=[VMEM] * (4 + len(arrivals)),
        out_specs=[VMEM] * 4,
        out_shape=[state] * 3 + [struct((rows, width_out), BF16)],
        scratch_shapes=[pltpu.VMEM((own_rows, lane), F32)],
        name="adam",
    )(*near(kept, *arrivals), master, moment, second)
    line = pl.pallas_call(
        functools.partial(stack_kernel, "gy"),
        in_specs=[VMEM] * nz,
        out_specs=VMEM,
        out_shape=struct((nz, rows, width_out), BF16),
        name="stack_line",
    )(*near(weights, *[permute(weights, dz=k) for k in range(1, nz)]))
    own = lax.all_gather(line, ("gx", "gr"), axis=0)
    out = pl.pallas_call(
        functools.partial(place_kernel, sizes, rows),
        in_specs=[VMEM] * 2,
        out_specs=ANY,
        out_shape=jax.ShapeDtypeStruct((width_in, width_out), BF16),
        scratch_shapes=[pltpu.SemaphoreType.DMA],
        name="place",
    )(*near(own, permute(own, dc=1)))
    return master_new, moment_new, second_new, out


def power_of_two(n):
    return n & (n - 1) == 0


def chosen(mesh, sizes, *args):
    acts, grads_out, master = args[:3]
    width_in, width_out = acts.shape[1], grads_out.shape[1]
    even = all(power_of_two(n) for n in sizes) and mesh.shape["gz"] % 2 == 0
    whole = width_in % (8 * mesh.size) == 0 and width_out % master.shape[1] == 0
    if not (even and whole):
        spec = P(AXES, None)
        return jax.shard_map(
            shards, mesh=mesh, in_specs=(spec,) * 5,
            out_specs=(spec,) * 3 + (P(),), check_vma=False,
        )(*args)
    spec = P(SPLIT, None)
    finer = Mesh(mesh.devices.reshape(*sizes, 2), SPLIT)
    return jax.shard_map(
        functools.partial(fast, sizes), mesh=finer, in_specs=(spec,) * 5,
        out_specs=(spec,) * 3 + (P(),), check_vma=False,
    )(*args)


def solution(mesh):
    sizes = (mesh.shape["gx"], mesh.shape["gy"], mesh.shape["gz"] // 2)
    return functools.partial(chosen, mesh, sizes)
```
